32 devices in a mesh: light: 4 (over y, x), screen: 8 (over z, core).
Axes of the slice: x: 2, y: 2, z: 4, core: 2. Of those that a mesh axis runs over, the one named last changes fastest.
Arguments:
- density: float32 [128, 256, 512], P('screen', None, 'light'), may hold values from 0 to 1.09375, as said below
- albedo: float32 [128, 256, 512], P('screen', None, 'light'), may hold values from 0.2 to 1
- light_in: float32 [128, 256], replicated, may hold values from 0.5 to 1.5
- occupancy: int32 [8, 16, 32], P('screen', None, 'light'), may hold values 0 or 1
- phase: int32 [256, 512], replicated, may hold values from 0 to 15
- fractions: float32 [3, 16], replicated, may hold values from 0 to 1
Outputs:
- image: float32 [256, 512], P('screen', 'light')
- transmittance: float32 [256, 512], P('screen', 'light')
- lit_bricks: float32 [128, 256, 512], P('light', 'screen')
The draws below stay inside these ranges and needn't reach their ends.
Inputs may be any that keep to these rules, and one draw needn't show every extreme that they name: `density`: nonnegative extinction of each cell. `occupancy`: 1 where the brick of 16 cells on a side is occupied.
All inputs are finite; a program needn't handle non-finite values. No bound on the sum of `occupancy` on one device may be relied on, other than what follows from the above.
Results may differ from the reference program's by a relative error of at most 0.0003.
Values sent between devices are 32-bit elements; how exact they have to be, the bound alone decides.
No kernel may reach another device: no remote copies, remote signals or barrier semaphores. Data moves between devices by JAX's collectives and lax.ppermute only.
A program may use at most 192 MiB of HBM per device.

```python
import math
import jax
import jax.numpy as jnp
from jax import lax

BRICK = 16
PHASES = 16
NL = 512
NA = 256
NB = 128


def draw_density(key, part):
    key_rate, key_rough, key_plane, key_patch, key_sheet = jax.random.split(key, 5)
    rate = jnp.exp(jax.random.uniform(key_rate, (NB, NA, 1), jnp.float32, math.log(0.2), math.log(6.0)))
    rough = jnp.exp(jax.random.uniform(key_rough, (NB, NA, NL), jnp.float32, math.log(0.02), math.log(50.0))) / 6.39
    planes = jax.random.randint(key_plane, (3,), 0, NL)
    on_plane = jnp.any(jnp.arange(NL)[None, :] == planes[:, None], axis=0).astype(jnp.float32)
    patch = (jax.random.uniform(key_patch, (NB, NA, NL), jnp.float32) < 0.5).astype(jnp.float32)
    sheet = jax.random.uniform(key_sheet, (NB, NA, NL), jnp.float32, 0.2, 0.7) * patch * on_plane[None, None, :]
    return rate * rough / NL + sheet


def place_ends(entries, own_key, low, top_value):
    extent = entries.shape
    spot = [jax.random.randint(jax.random.fold_in(own_key, axis), (), 0, extent[axis]) for axis in range(len(extent))]
    entries = entries.at[tuple(spot)].set(low)
    longest = extent.index(max(extent))
    spot[longest] = (spot[longest] + 1) % extent[longest]
    return entries.at[tuple(spot)].set(top_value)


def steps_of(rng, dims, shards, smallest, high):
    level = 1.0
    for dim, shards_of in shards:
        draws = jax.random.uniform(jax.random.fold_in(jax.random.fold_in(rng, 6), dim), (shards_of,), jnp.float32, smallest / len(shards), high / len(shards))
        level = level * jnp.repeat(jnp.exp(draws), dims[dim] // shards_of).reshape((-1,) + (1,) * (len(dims) - 1 - dim))
    return level


def setup_inputs(seed: int = 0) -> dict:
    arg_keys = jax.random.split(jax.random.key(seed), 7)
    density = draw_density(jax.random.fold_in(arg_keys[6], 71), 0)
    albedo = jnp.clip(0.2 + 0.8 * jax.random.uniform(arg_keys[1], (NB, NA, NL), jnp.float32) ** steps_of(arg_keys[1], (NB, NA, NL), ((0, 8), (2, 4)), -0.2, 0.2), 0.2, 1.0)
    light_in = jnp.clip(jax.random.uniform(arg_keys[2], (NB, NA), jnp.float32, 0.5, 1.5), 0.5, 1.5)
    occupancy = place_ends((jax.random.randint(arg_keys[3], (NB // BRICK, NA // BRICK, NL // BRICK), 0, 4) < 3).astype(jnp.int32), jax.random.fold_in(arg_keys[3], 1), 0, 1)
    phase = place_ends(jax.random.randint(arg_keys[4], (NA, NL), 0, PHASES), jax.random.fold_in(arg_keys[4], 1), 0, PHASES - 1).astype(jnp.int32)
    fractions = jnp.clip(jax.random.uniform(arg_keys[5], (3, PHASES), jnp.float32, 0.0, 1.0), 0.0, 1.0)
    return {"density": density, "albedo": albedo, "light_in": light_in, "occupancy": occupancy, "phase": phase, "fractions": fractions}


def reference(density, albedo, light_in, occupancy, phase, fractions):
    bricks_b, bricks_a, bricks_l = occupancy.shape
    masked = (density.reshape(bricks_b, BRICK, bricks_a, BRICK, bricks_l, BRICK)
              * occupancy.astype(jnp.float32)[:, None, :, None, :, None]).reshape(density.shape)
    light_depth = jnp.cumsum(masked, axis=2) - masked
    lit_bricks = albedo * light_in[:, :, None] * jnp.exp(-light_depth)
    volumes = jnp.stack([masked, lit_bricks])
    padded = jnp.pad(volumes, ((0, 0), (0, 2), (0, 2), (0, 1)))
    weights = fractions[:, phase]
    tiles = NA // BRICK

    def render(tile):
        zero = jnp.zeros((), jnp.int32)
        start = (tile * BRICK).astype(jnp.int32)
        block = lax.dynamic_slice(padded, (zero, zero, start, zero), (2, NB + 2, BRICK + 2, NL + 1))
        tile_w = lax.dynamic_slice(weights, (zero, start, zero), (3, BRICK, NL))
        sampled = jnp.zeros((2, NB, BRICK, NL), jnp.float32)
        for corner_b in (0, 1):
            for corner_a in (0, 1):
                for corner_l in (0, 1):
                    factor = tile_w[0] if corner_b else 1.0 - tile_w[0]
                    factor = factor * (tile_w[1] if corner_a else 1.0 - tile_w[1])
                    factor = factor * (tile_w[2] if corner_l else 1.0 - tile_w[2])
                    piece = block[:, corner_b:corner_b + NB, corner_a:corner_a + BRICK, corner_l:corner_l + NL]
                    sampled = sampled + factor * piece
        extinct = sampled[0]
        shaded = sampled[1]
        screened = jnp.cumsum(extinct, axis=0) - extinct
        picture = jnp.sum(jnp.exp(-screened) * (1.0 - jnp.exp(-extinct)) * shaded, axis=0)
        passing = jnp.exp(-jnp.sum(extinct, axis=0))
        return picture, passing

    pictures, passings = lax.map(render, jnp.arange(tiles, dtype=jnp.int32))
    return pictures.reshape(NA, NL), passings.reshape(NA, NL), lit_bricks
```

```python
import functools

import jax
import jax.numpy as jnp
from jax import lax
from jax.experimental import pallas as pl
from jax.experimental.pallas import tpu as pltpu
from jax.sharding import PartitionSpec as P


BRICK = 16
SUB = 8


def bit_reversed(value, size):
    out = 0
    bit = 1
    while bit < size:
        out = out * 2 + ((value // bit) & 1 if isinstance(value, int) else lax.div(value, bit) & 1)
        bit *= 2
    return out


def over(value, by):
    return value // by if isinstance(value, int) else lax.div(value, by)


def rounds_of(lights, screens):
    per = screens // lights
    return [(step, core) for core in range(per) for step in range(lights)]


def target_screen(light, screen, rnd, lights, screens):
    per = screens // lights
    step, core = rnd
    return (bit_reversed(over(screen, per), lights) ^ light ^ step) * per + ((screen & (per - 1)) ^ core)


def source_of(light, screen, rnd, lights, screens):
    per = screens // lights
    step, core = rnd
    return bit_reversed(light, lights) ^ over(screen, per) ^ step, (screen & (per - 1)) ^ core


def round_pairs(rnd, lights, screens):
    per = screens // lights
    pairs = []
    for light in range(lights):
        for screen in range(screens):
            there = (screen // per) * screens + target_screen(light, screen, rnd, lights, screens)
            pairs.append((light * screens + screen, there))
    return pairs


def brick_rows(occ_ref, out, width):
    bricks = occ_ref.shape[1]
    here = lax.broadcasted_iota(jnp.int32, (bricks, width), 1) // BRICK
    spread = (here == lax.broadcasted_iota(jnp.int32, (bricks, width), 0)).astype(jnp.float32)
    flags = occ_ref[0].astype(jnp.float32)
    out[...] = lax.dot_general(flags, spread, (((0,), (0,)), ((), ())), preferred_element_type=jnp.float32)


def halves(values):
    high = values.astype(jnp.bfloat16)
    low = (values - high.astype(jnp.float32)).astype(jnp.bfloat16)
    return jnp.concatenate([high, low], axis=-1)


def prefix_matrix(width, with_total):
    rows = lax.broadcasted_iota(jnp.int32, (2 * width, (1 + with_total) * width), 0) % width
    cols = lax.broadcasted_iota(jnp.int32, (2 * width, (1 + with_total) * width), 1)
    return (rows < cols).astype(jnp.float32).astype(jnp.bfloat16)


def chunk_kernel(count, spot_of, first, has_small, *refs):
    occ_ref, density_ref, albedo_ref = refs[:3]
    outs = refs[3 + has_small : -3]
    small_ref, brick, tri = refs[-3:]
    step = pl.program_id(0)
    depth, rows, width = density_ref.shape

    @pl.when(step == 0)
    def _():
        brick_rows(occ_ref, brick, width)
        tri[...] = prefix_matrix(width, 1)

    bands = rows // BRICK
    spot = spot_of(first + step)
    mask = jnp.concatenate(
        [jnp.broadcast_to(brick[pl.ds(spot * bands + band, 1), :], (BRICK, width)) for band in range(bands)], axis=0
    )
    masked = (density_ref[...] * mask[None]).reshape(depth * rows, width)
    sums = jnp.dot(halves(masked), tri[...], preferred_element_type=jnp.float32)
    within = jnp.exp(-sums[:, :width])
    total = sums[:, width:]
    albedo = albedo_ref[...].reshape(depth * rows, width)
    lane = lax.broadcasted_iota(jnp.int32, (SUB, width), 1)
    packed = [jnp.zeros((SUB, width), jnp.float32)] * 3
    for b in range(depth):
        for group in range(rows // SUB):
            at = b * rows + group * SUB
            here = lane == group * depth + b
            packed[0] = jnp.where(here, total[at : at + SUB], packed[0])
            packed[1] = jnp.where(here, masked[at : at + SUB, 0:1], packed[1])
            packed[2] = jnp.where(here, albedo[at : at + SUB, 0:1], packed[2])
    for kind in range(3):
        small_ref[kind] = packed[kind]
    lit = albedo * within
    for index in range(count):

        @pl.when(step == index)
        def _():
            outs[index][: depth * rows, :] = lit
            outs[index][depth * rows :, :] = packed[0]


def lit_chunks(density, albedo, occupancy, spot_of, first, count, screens, small):
    depth, width_a, width = density.shape
    rows = width_a // screens
    spec = pl.BlockSpec((depth, rows, width), lambda i: (0, spot_of(first + i), 0))
    size = depth * rows + SUB
    has_small = small is not None
    return pl.pallas_call(
        functools.partial(chunk_kernel, count, spot_of, first, int(has_small)),
        grid=(count,),
        in_specs=[pl.BlockSpec(occupancy.shape, lambda i: (0, 0, 0)), spec, spec]
        + [pl.BlockSpec(memory_space=pl.ANY)] * has_small,
        out_specs=[pl.BlockSpec((size, width), lambda i: (0, 0))] * count
        + [pl.BlockSpec((3, SUB, width), lambda i: (0, spot_of(first + i), 0))],
        out_shape=[jax.ShapeDtypeStruct((size, width), jnp.float32)] * count
        + [jax.ShapeDtypeStruct((3, SUB * screens, width), jnp.float32)],
        scratch_shapes=[
            pltpu.VMEM((occupancy.shape[2], width), jnp.float32),
            pltpu.VMEM((2 * width, 2 * width), jnp.bfloat16),
        ],
        input_output_aliases={3: count} if has_small else {},
        compiler_params=pltpu.CompilerParams(vmem_limit_bytes=CHUNK_VMEM),
        cost_estimate=pl.CostEstimate(flops=10**7 * count, bytes_accessed=3 * size * width * 4 * count, transcendentals=0),
        name="lit_chunks",
    )(occupancy, density, albedo, *([small] if has_small else []))


CHUNK_VMEM = 56 << 20
MARCH_VMEM = 56 << 20


def gather_kernel(depth, lights, place_of, light_ref, *refs):
    count = len(refs) - 4
    chunks = refs[:count]
    out_ref, held, totals, sem = refs[count:]
    size, width = chunks[0].shape
    rows = (size - SUB) // depth
    for j in range(count):
        light, place = place_of(j)
        totals[place, light] = chunks[j][size - SUB :, :]
    copies = []
    for j in range(count):
        light, place = place_of(j)
        before = jnp.zeros((SUB, width), jnp.float32)
        for other in range(lights - 1):
            before = before + jnp.where(other < light, totals[place, other], 0.0)
        factor = light_ref[place] * jnp.exp(-before)
        for b in range(depth):
            for group in range(rows // SUB):
                at = b * rows + group * SUB
                lane = group * depth + b
                held[j, b, group * SUB : (group + 1) * SUB, :] = chunks[j][at : at + SUB, :] * factor[:, lane : lane + 1]
        copy = pltpu.make_async_copy(
            held.at[j],
            out_ref.at[pl.ds(place * depth, depth), :, pl.ds(pl.multiple_of(light * width, width), width)],
            sem.at[j],
        )
        copy.start()
        copies.append(copy)
    for copy in copies:
        copy.wait()


def gather_block(chunks, incoming, place_of, depth, lights, per):
    size, width = chunks[0].shape
    rows = (size - SUB) // depth
    return pl.pallas_call(
        functools.partial(gather_kernel, depth, lights, place_of),
        in_specs=[pl.BlockSpec(memory_space=pltpu.VMEM)] * (1 + len(chunks)),
        out_specs=pl.BlockSpec(memory_space=pl.ANY),
        out_shape=jax.ShapeDtypeStruct((per * depth, rows, lights * width), jnp.float32),
        scratch_shapes=[
            pltpu.VMEM((len(chunks), depth, rows, width), jnp.float32),
            pltpu.VMEM((per, lights, SUB, width), jnp.float32),
            pltpu.SemaphoreType.DMA((len(chunks),)),
        ],
        compiler_params=pltpu.CompilerParams(vmem_limit_bytes=24 << 20),
        name="gather_block",
    )(incoming, *chunks)


def march_kernel(
    lights, occ_ref, frac_ref, density_ref, albedo_ref, light_ref, small_ref, *refs
):
    others = refs[: lights - 1]
    phase_ref, first_ref, state_ref, weight_ref, brick, mask, columns, mixes, front, tri, field = refs[lights - 1 :]
    b = pl.program_id(0)
    depth = pl.num_programs(0)
    _, width_a, width = density_ref.shape
    steps = light_ref.shape[1]

    @pl.when(b == 0)
    def _():
        brick_rows(occ_ref, brick, width)
        for row in range(width_a // BRICK):
            mask[row * BRICK : (row + 1) * BRICK, :] = jnp.broadcast_to(brick[row : row + 1, :], (BRICK, width))
        levels = phase_ref[...]
        for axis in range(3):
            weight = jnp.zeros((width_a, width), jnp.float32)
            for level in range(frac_ref.shape[1]):
                weight = jnp.where(levels == level, frac_ref[axis, level], weight)
            weight_ref[axis] = weight
        tri[...] = prefix_matrix(width, 0)
        light = lax.axis_index("light")
        near = jnp.zeros(small_ref.shape[1:], jnp.float32)
        next_m = jnp.zeros(small_ref.shape[1:], jnp.float32)
        next_a = jnp.zeros(small_ref.shape[1:], jnp.float32)
        for by in range(1, lights):
            other = light ^ by
            near = near + jnp.where(other < light, others[by - 1][0], 0.0)
            next_m = next_m + jnp.where(other == light + 1, others[by - 1][1], 0.0)
            next_a = next_a + jnp.where(other == light + 1, others[by - 1][2], 0.0)
        far = jnp.exp(-(near + small_ref[0])) * next_a
        near = jnp.exp(-near)
        chunks = near.shape[0] // SUB
        groups = width_a // chunks // SUB
        pad = jnp.zeros((SUB, width - steps), jnp.float32)
        for chunk in range(chunks):
            for group in range(groups):
                at = (chunk * groups + group) * SUB
                back = (width - group * steps) % width

                def turned(x):
                    tile = x[chunk * SUB : (chunk + 1) * SUB]
                    return pltpu.roll(tile, back, 1) if back else tile

                incoming = jnp.concatenate([light_ref[at : at + SUB, :], pad], axis=1)
                columns[0, at : at + SUB, :] = incoming * turned(near)
                columns[1, at : at + SUB, :] = turned(next_m)
                columns[2, at : at + SUB, :] = incoming * turned(far)
        state_ref[...] = jnp.zeros_like(state_ref)
        front[...] = jnp.ones_like(front)
        mixes[...] = jnp.zeros_like(mixes)
        field[:, width_a:, :] = jnp.zeros((4, SUB, width), jnp.float32)

    lane = lax.broadcasted_iota(jnp.int32, (width_a, width), 1)
    masked = density_ref[0] * mask[...]
    within = jnp.dot(halves(masked), tri[...], preferred_element_type=jnp.float32)
    lit = albedo_ref[0] * columns[0][:, 0:1] * jnp.exp(-within)
    field[0, :width_a, :] = masked
    field[1, :width_a, :] = lit
    field[2, :width_a, :] = jnp.where(lane == width - 1, columns[1][:, 0:1], pltpu.roll(masked, width - 1, 1))
    field[3, :width_a, :] = jnp.where(lane == width - 1, columns[2][:, 0:1], pltpu.roll(lit, width - 1, 1))
    for kind in range(3):
        columns[kind] = pltpu.roll(columns[kind], width - 1, 1)

    for start in range(0, width_a, BAND):
        at = slice(start, start + BAND)
        below = slice(start + 1, start + BAND + 1)
        depth_w = weight_ref[0, at, :]
        column_w = weight_ref[1, at, :]
        light_w = weight_ref[2, at, :]

        def mixed(kind):
            near = field[kind, at, :]
            near = near + column_w * (field[kind, below, :] - near)
            after = field[kind + 2, at, :]
            after = after + column_w * (field[kind + 2, below, :] - after)
            return near + light_w * (after - near)

        mix_m = mixed(0)
        mix_s = mixed(1)
        old_m = mixes[0, at, :]
        old_s = mixes[1, at, :]
        extinct = old_m + depth_w * (mix_m - old_m)
        shaded = old_s + depth_w * (mix_s - old_s)
        extinct = jnp.where(b > 0, extinct, 0.0)
        total = state_ref[1, at, :] + extinct
        left = jnp.exp(-total)
        state_ref[0, at, :] = state_ref[0, at, :] + (front[at, :] - left) * shaded
        state_ref[1, at, :] = total
        front[at, :] = left
        mixes[0, at, :] = mix_m
        mixes[1, at, :] = mix_s

    @pl.when(b == 0)
    def _():
        first_ref[...] = mixes[...]

    @pl.when(b == depth - 1)
    def _():
        state_ref[2:] = mixes[...]


BAND = 64


def march(density, albedo, light_cols, occupancy, fractions, small, others, rays):
    depth, width_a, width = density.shape
    spec = pl.BlockSpec((1, width_a, width), lambda b: (b, 0, 0))

    def whole(x):
        return pl.BlockSpec(x.shape, lambda b: (0,) * x.ndim)

    shapes = [(2, width_a, width), (4, width_a, width), (3, width_a, width)]
    return pl.pallas_call(
        functools.partial(march_kernel, len(others) + 1),
        grid=(depth,),
        in_specs=[whole(occupancy), pl.BlockSpec(memory_space=pltpu.SMEM), spec, spec]
        + [whole(x) for x in (light_cols, small, *others, rays)],
        out_specs=[pl.BlockSpec(s, lambda b: (0, 0, 0)) for s in shapes],
        scratch_shapes=[
            pltpu.VMEM((occupancy.shape[2], width), jnp.float32),
            pltpu.VMEM((width_a, width), jnp.float32),
            pltpu.VMEM((3, width_a, width), jnp.float32),
            pltpu.VMEM((2, width_a, width), jnp.float32),
            pltpu.VMEM((width_a, width), jnp.float32),
            pltpu.VMEM((2 * width, width), jnp.bfloat16),
            pltpu.VMEM((4, width_a + SUB, width), jnp.float32),
        ],
        out_shape=[jax.ShapeDtypeStruct(s, jnp.float32) for s in shapes],
        compiler_params=pltpu.CompilerParams(vmem_limit_bytes=MARCH_VMEM),
        cost_estimate=pl.CostEstimate(flops=10**8, bytes_accessed=2 * depth * width_a * width * 4, transcendentals=0),
        name="march",
    )(occupancy, fractions, density, albedo, light_cols, small, *others, rays)


def shifted(value, axis, by):
    peers = lax.axis_size(axis)
    return lax.ppermute(value, axis, [(i, i + by) for i in range(peers) if 0 <= i + by < peers])


def swapped(value, axis, by):
    peers = lax.axis_size(axis)
    return lax.ppermute(value, axis, [(i, i ^ by) for i in range(peers)])


def step(density, albedo, light_in, occupancy, phase, fractions):
    depth, width_a, width = density.shape
    lights, screens = lax.axis_size("light"), lax.axis_size("screen")
    light, screen = lax.axis_index("light"), lax.axis_index("screen")
    per = screens // lights
    rows = width_a // screens
    rounds = rounds_of(lights, screens)
    pairs = [round_pairs(rnd, lights, screens) for rnd in rounds]

    def spot_of(j):
        here = lax.axis_index("light"), lax.axis_index("screen")
        return target_screen(*here, (lax.rem(j, lights), lax.div(j, lights)), lights, screens)

    def place_of(j):
        return source_of(lax.axis_index("light"), lax.axis_index("screen"), rounds[j], lights, screens)

    def send(j, chunk):
        return lax.ppermute(chunk, ("light", "screen"), pairs[j])

    count = len(rounds)
    flags = occupancy.transpose(0, 2, 1)
    early = lit_chunks(density, albedo, flags, spot_of, 0, 2, screens, None)
    late = lit_chunks(density, albedo, flags, spot_of, 2, count - 2, screens, early[-1])
    small = late[-1]
    arrived = [send(j, chunk) for j, chunk in enumerate(early[:2] + late[:-1])]

    others = [swapped(small, "light", by) for by in range(1, lights)]
    light_cols = lax.dynamic_slice_in_dim(light_in, screen * depth, depth, 0).T
    rays = lax.dynamic_slice_in_dim(phase, light * width, width, 1)
    first, state, weights = march(density, albedo, light_cols, flags, fractions, small, others, rays)
    behind = shifted(first, "screen", -1)
    extinct = state[2] + weights[0] * (behind[0] - state[2])
    shaded = state[3] + weights[0] * (behind[1] - state[3])
    total = state[1] + extinct
    part = state[0] + (jnp.exp(-state[1]) - jnp.exp(-total)) * shaded

    pair = jnp.stack([part, total]).reshape(2, screens // 2, 2, rows, width)
    core = screen % 2
    mine = lax.dynamic_index_in_dim(pair, core, 2, False)
    theirs = lax.dynamic_index_in_dim(pair, 1 - core, 2, False)
    other = swapped(theirs, "screen", 1)
    closer = jnp.where(core == 0, mine, other)
    farther = jnp.where(core == 0, other, mine)
    joined = jnp.stack([closer[0] + jnp.exp(-closer[1]) * farther[0], closer[1] + farther[1]])
    place = screen // 2
    got = [lax.dynamic_index_in_dim(joined, place, 1, False)]
    for by in range(1, screens // 2):
        piece = lax.dynamic_index_in_dim(joined, place ^ by, 1, False)
        got.append(swapped(piece, "screen", 2 * by))
    image = jnp.zeros((rows, width), jnp.float32)
    through = jnp.zeros((rows, width), jnp.float32)
    for by, (shine, thick) in enumerate(got):
        ahead = jnp.zeros((rows, width), jnp.float32)
        for other_by, (_, other_thick) in enumerate(got):
            if other_by != by:
                ahead = ahead + jnp.where((place ^ other_by) < (place ^ by), other_thick, 0.0)
        image = image + jnp.exp(-ahead) * shine
        through = through + thick
    incoming = lax.dynamic_slice(light_in, (light * per * depth, screen * rows), (per * depth, rows))
    incoming = incoming.reshape(per, depth, rows // SUB, SUB).transpose(0, 3, 2, 1).reshape(per, SUB, rows // SUB * depth)
    incoming = jnp.pad(incoming, ((0, 0), (0, 0), (0, width - incoming.shape[2])))
    lit_bricks = gather_block(arrived, incoming, place_of, depth, lights, per)
    return image, jnp.exp(-through), lit_bricks


def solution(mesh):
    return jax.shard_map(
        step,
        mesh=mesh,
        in_specs=(
            P("screen", None, "light"),
            P("screen", None, "light"),
            P(),
            P("screen", None, "light"),
            P(),
            P(),
        ),
        out_specs=(P("screen", "light"), P("screen", "light"), P("light", "screen", None)),
        check_vma=False,
    )
```

```python
import functools

import jax
import jax.numpy as jnp
from jax import lax
from jax.experimental import pallas as pl
from jax.experimental.pallas import tpu as pltpu
from jax.sharding import PartitionSpec as P


BRICK = 16
SUB = 8


def bit_reversed(value, size):
    out = 0
    bit = 1
    while bit < size:
        out = out * 2 + ((value // bit) & 1 if isinstance(value, int) else lax.div(value, bit) & 1)
        bit *= 2
    return out


def over(value, by):
    return value // by if isinstance(value, int) else lax.div(value, by)


def rounds_of(lights, screens):
    per = screens // lights
    return [(step, core) for core in range(per) for step in range(lights)]


def target_screen(light, screen, rnd, lights, screens):
    per = screens // lights
    step, core = rnd
    return (bit_reversed(over(screen, per), lights) ^ light ^ step) * per + ((screen & (per - 1)) ^ core)


def source_of(light, screen, rnd, lights, screens):
    per = screens // lights
    step, core = rnd
    return bit_reversed(light, lights) ^ over(screen, per) ^ step, (screen & (per - 1)) ^ core


def round_pairs(rnd, lights, screens):
    per = screens // lights
    pairs = []
    for light in range(lights):
        for screen in range(screens):
            there = (screen // per) * screens + target_screen(light, screen, rnd, lights, screens)
            pairs.append((light * screens + screen, there))
    return pairs


def brick_rows(occ_ref, out, width):
    bricks = occ_ref.shape[1]
    here = lax.broadcasted_iota(jnp.int32, (bricks, width), 1) // BRICK
    spread = (here == lax.broadcasted_iota(jnp.int32, (bricks, width), 0)).astype(jnp.float32)
    flags = occ_ref[0].astype(jnp.float32)
    out[...] = lax.dot_general(flags, spread, (((0,), (0,)), ((), ())), preferred_element_type=jnp.float32)


def halves(values):
    high = values.astype(jnp.bfloat16)
    low = (values - high.astype(jnp.float32)).astype(jnp.bfloat16)
    return jnp.concatenate([high, low], axis=-1)


def prefix_matrix(width, with_total):
    rows = lax.broadcasted_iota(jnp.int32, (2 * width, (1 + with_total) * width), 0) % width
    cols = lax.broadcasted_iota(jnp.int32, (2 * width, (1 + with_total) * width), 1)
    return (rows < cols).astype(jnp.float32).astype(jnp.bfloat16)


def chunk_kernel(count, spot_of, first, *refs):
    occ_any, density_ref, albedo_ref = refs[:3]
    before = refs[3 : 3 + bool(first)]
    rest = refs[3 + bool(first) :]
    outs = rest[:count]
    brims = rest[count : -7]
    small_ref, occ_ref, brick, tri, density, albedo, sem = rest[-7:]
    _, depth, rows, width = density.shape

    def fetches(k):
        columns = pl.ds(spot_of(first + k) * rows, rows)
        return (
            pltpu.make_async_copy(density_ref.at[:, columns, :], density.at[k], sem.at[0, k]),
            pltpu.make_async_copy(albedo_ref.at[:, columns, :], albedo.at[k], sem.at[1, k]),
        )

    flags = pltpu.make_async_copy(occ_any, occ_ref, sem.at[2, 0])
    flags.start()
    for k in range(count):
        for fetch in fetches(k):
            fetch.start()
    for brim in brims:
        pltpu.make_async_copy(density_ref.at[0], brim.at[0], sem.at[2, 1]).start()
        pltpu.make_async_copy(albedo_ref.at[0], brim.at[1], sem.at[2, 2]).start()
    tri[...] = prefix_matrix(width, 1)
    flags.wait()
    brick_rows(occ_ref, brick, width)
    bands = rows // BRICK
    lane = lax.broadcasted_iota(jnp.int32, (SUB, width), 1)
    for k in range(count):
        spot = spot_of(first + k)
        mask = jnp.concatenate(
            [jnp.broadcast_to(brick[pl.ds(spot * bands + band, 1), :], (BRICK, width)) for band in range(bands)], axis=0
        )
        for fetch in fetches(k):
            fetch.wait()
        packed = [jnp.zeros((SUB, width), jnp.float32)] * 3
        for b in range(depth):
            masked = density[k, b] * mask
            sums = jnp.dot(halves(masked), tri[...], preferred_element_type=jnp.float32)
            light = albedo[k, b]
            outs[k][b * rows : (b + 1) * rows, :] = light * jnp.exp(-sums[:, :width])
            for group in range(rows // SUB):
                at = slice(group * SUB, (group + 1) * SUB)
                here = lane == group * (depth + 1) + b
                packed[0] = jnp.where(here, sums[at, width:], packed[0])
                packed[1] = jnp.where(here, masked[at, 0:1], packed[1])
                packed[2] = jnp.where(here, light[at, 0:1], packed[2])
        outs[k][depth * rows :, :] = packed[0]
        tile = pl.multiple_of(spot * SUB, SUB) if first else k * SUB
        for kind in range(3):
            small_ref[kind, pl.ds(tile, SUB), :] = packed[kind]
    for brim in brims:
        pltpu.make_async_copy(density_ref.at[0], brim.at[0], sem.at[2, 1]).wait()
        pltpu.make_async_copy(albedo_ref.at[0], brim.at[1], sem.at[2, 2]).wait()
        for row in range(brick.shape[0]):
            at = slice(row * BRICK, (row + 1) * BRICK)
            brim[0, at, :] = brim[0, at, :] * brick[row : row + 1, :]
    for held in before:
        for k in range(first):
            tile = pl.multiple_of(spot_of(k) * SUB, SUB)
            small_ref[:, pl.ds(tile, SUB), :] = held[:, k * SUB : (k + 1) * SUB, :]


def lit_chunks(density, albedo, occupancy, spot_of, first, count, screens, *before):
    depth, width_a, width = density.shape
    rows = width_a // screens
    size = depth * rows + SUB
    vmem = pl.BlockSpec(memory_space=pltpu.VMEM)
    tiles = screens if before else count
    brim = [] if before else [jax.ShapeDtypeStruct((2, width_a, width), jnp.float32)]
    return pl.pallas_call(
        functools.partial(chunk_kernel, count, spot_of, first),
        in_specs=[pl.BlockSpec(memory_space=pl.ANY)] * 3 + [vmem] * len(before),
        out_specs=[vmem] * (count + 1 + len(brim)),
        out_shape=[jax.ShapeDtypeStruct((size, width), jnp.float32)] * count
        + brim
        + [jax.ShapeDtypeStruct((3, SUB * tiles, width), jnp.float32)],
        scratch_shapes=[
            pltpu.VMEM(occupancy.shape, occupancy.dtype),
            pltpu.VMEM((occupancy.shape[2], width), jnp.float32),
            pltpu.VMEM((2 * width, 2 * width), jnp.bfloat16),
            pltpu.VMEM((count, depth, rows, width), jnp.float32),
            pltpu.VMEM((count, depth, rows, width), jnp.float32),
            pltpu.SemaphoreType.DMA((3, max(count, 3))),
        ],
        compiler_params=pltpu.CompilerParams(vmem_limit_bytes=CHUNK_VMEM),
        cost_estimate=pl.CostEstimate(flops=10**7 * count, bytes_accessed=3 * size * width * 4 * count, transcendentals=0),
        name="lit_chunks",
    )(occupancy, density, albedo, *before)


CHUNK_VMEM = 12 << 20
MARCH_VMEM = 16 << 20


def rim_kernel(depth, small_ref, brim_ref, out_ref):
    _, width_a, width = brim_ref.shape
    tiles = small_ref.shape[1] // SUB
    groups = width_a // tiles // SUB
    masked = brim_ref[0]
    light = brim_ref[1]
    total = jnp.dot(halves(masked), jnp.ones((2 * width, width), jnp.bfloat16), preferred_element_type=jnp.float32)
    lane = lax.broadcasted_iota(jnp.int32, (SUB, width), 1)
    for tile in range(tiles):
        rows = slice(tile * SUB, (tile + 1) * SUB)
        packed = [small_ref[kind, rows, :] for kind in range(3)]
        for group in range(groups):
            at = slice((tile * groups + group) * SUB, (tile * groups + group + 1) * SUB)
            here = lane == group * (depth + 1) + depth
            packed[0] = jnp.where(here, total[at], packed[0])
            packed[1] = jnp.where(here, masked[at, 0:1], packed[1])
            packed[2] = jnp.where(here, light[at, 0:1], packed[2])
        for kind in range(3):
            out_ref[kind, rows, :] = packed[kind]


def with_rim(small, brim, depth):
    vmem = pl.BlockSpec(memory_space=pltpu.VMEM)
    return pl.pallas_call(
        functools.partial(rim_kernel, depth),
        in_specs=[vmem] * 2,
        out_specs=vmem,
        out_shape=jax.ShapeDtypeStruct(small.shape, jnp.float32),
        compiler_params=pltpu.CompilerParams(vmem_limit_bytes=4 << 20),
        cost_estimate=pl.CostEstimate(flops=10**6, bytes_accessed=10**6, transcendentals=0),
        name="rim",
    )(small, brim)


def gather_kernel(depth, lights, place_of, light_ref, parts_ref, *refs):
    count = len(refs) - 6
    chunks = refs[:count]
    image_ref, through_ref, out_ref, held, totals, sem = refs[count:]
    size, width = chunks[0].shape
    rows = (size - SUB) // depth
    for j in range(count):
        light, place = place_of(j)
        totals[place, light] = chunks[j][size - SUB :, :]
    copies = []
    for j in range(count):
        light, place = place_of(j)
        before = jnp.zeros((SUB, width), jnp.float32)
        for other in range(lights - 1):
            before = before + jnp.where(other < light, totals[place, other], 0.0)
        factor = light_ref[place] * jnp.exp(-before)
        for b in range(depth):
            for group in range(rows // SUB):
                at = b * rows + group * SUB
                lane = group * (depth + 1) + b
                held[j, b, group * SUB : (group + 1) * SUB, :] = chunks[j][at : at + SUB, :] * factor[:, lane : lane + 1]
        copy = pltpu.make_async_copy(
            held.at[j],
            out_ref.at[pl.ds(place * depth, depth), :, pl.ds(pl.multiple_of(light * width, width), width)],
            sem.at[j],
        )
        copy.start()
        copies.append(copy)
    image = jnp.zeros(image_ref.shape, jnp.float32)
    ahead = jnp.zeros(image_ref.shape, jnp.float32)
    for slab in range(parts_ref.shape[0]):
        image = image + jnp.exp(-ahead) * parts_ref[slab, 0]
        ahead = ahead + parts_ref[slab, 1]
    image_ref[...] = image
    through_ref[...] = jnp.exp(-ahead)
    for copy in copies:
        copy.wait()


def gather_block(chunks, parts, incoming, place_of, depth, lights, per):
    size, width = chunks[0].shape
    rows = (size - SUB) // depth
    return pl.pallas_call(
        functools.partial(gather_kernel, depth, lights, place_of),
        in_specs=[pl.BlockSpec(memory_space=pltpu.VMEM)] * (2 + len(chunks)),
        out_specs=[pl.BlockSpec(memory_space=pltpu.VMEM)] * 2 + [pl.BlockSpec(memory_space=pl.ANY)],
        out_shape=[jax.ShapeDtypeStruct((rows, width), jnp.float32)] * 2
        + [jax.ShapeDtypeStruct((per * depth, rows, lights * width), jnp.float32)],
        scratch_shapes=[
            pltpu.VMEM((len(chunks), depth, rows, width), jnp.float32),
            pltpu.VMEM((per, lights, SUB, width), jnp.float32),
            pltpu.SemaphoreType.DMA((len(chunks),)),
        ],
        compiler_params=pltpu.CompilerParams(vmem_limit_bytes=24 << 20),
        name="gather_block",
    )(incoming, parts, *chunks)


BAND = 32


def march_kernel(lights, occ_any, frac_ref, density_ref, albedo_ref, light_any, brim_ref, small_ref, *refs):
    arriving = refs[: lights - 1]
    phase_ref, out_ref = refs[lights - 1 : lights + 1]
    state_ref, depth_ref, brick, mask, columns, edges, weights, front, tri, field = refs[lights + 1 : lights + 11]
    density, albedo, occ_ref, light_ref, others, sem = refs[lights + 11 :]
    depth, width_a, width = density.shape
    steps = light_ref.shape[1]

    def fetches(b):
        return (
            pltpu.make_async_copy(density_ref.at[b], density.at[b], sem.at[0, b]),
            pltpu.make_async_copy(albedo_ref.at[b], albedo.at[b], sem.at[1, b]),
        )

    early = [pltpu.make_async_copy(occ_any, occ_ref, sem.at[2, 0]), pltpu.make_async_copy(light_any, light_ref, sem.at[2, 1])]
    early += [pltpu.make_async_copy(ref, others.at[i], sem.at[2, 2 + i]) for i, ref in enumerate(arriving)]
    for copy in early:
        copy.start()
    for b in range(depth):
        for fetch in fetches(b):
            fetch.start()
    for start in range(0, width_a, BAND):
        at = slice(start, start + BAND)
        levels = phase_ref[at, :]
        picked = [jnp.zeros((BAND, width), jnp.float32)] * 3
        for level in range(frac_ref.shape[1]):
            here = levels == level
            picked = [jnp.where(here, frac_ref[axis, level], value) for axis, value in enumerate(picked)]
        depth_ref[at, :] = picked[0]
        far_w = picked[1] * picked[2]
        weights[0, at, :] = 1.0 - picked[1] - picked[2] + far_w
        weights[1, at, :] = picked[1] - far_w
        weights[2, at, :] = picked[2] - far_w
        weights[3, at, :] = far_w
    rows = lax.broadcasted_iota(jnp.int32, (2 * width, width), 0) % width
    above = rows < lax.broadcasted_iota(jnp.int32, (2 * width, width), 1)
    tri[...] = jnp.where(above | (rows == width - 1), 1.0, 0.0).astype(jnp.bfloat16)
    for copy in early:
        copy.wait()
    brick_rows(occ_ref, brick, width)
    for row in range(width_a // BRICK):
        mask[row * BRICK : (row + 1) * BRICK, :] = jnp.broadcast_to(brick[row : row + 1, :], (BRICK, width))
    light = lax.axis_index("light")
    near = jnp.zeros(small_ref.shape[1:], jnp.float32)
    next_m = jnp.zeros(small_ref.shape[1:], jnp.float32)
    next_a = jnp.zeros(small_ref.shape[1:], jnp.float32)
    for by in range(1, lights):
        other = light ^ by
        near = near + jnp.where(other < light, others[by - 1, 0], 0.0)
        next_m = next_m + jnp.where(other == light + 1, others[by - 1, 1], 0.0)
        next_a = next_a + jnp.where(other == light + 1, others[by - 1, 2], 0.0)
    far = jnp.exp(-(near + small_ref[0])) * next_a
    chunks = near.shape[0] // SUB
    groups = width_a // chunks // SUB
    lane = lax.broadcasted_iota(jnp.int32, (SUB, width), 1)
    tiles = [[], []]
    for chunk in range(chunks):
        for group in range(groups):
            at = (chunk * groups + group) * SUB
            back = (width - group * steps) % width

            def turned(x):
                tile = x[chunk * SUB : (chunk + 1) * SUB]
                return pltpu.roll(tile, back, 1) if back else tile

            incoming = jnp.concatenate([light_ref[at : at + SUB, :], jnp.ones((SUB, width - steps), jnp.float32)], axis=1)
            edges[at : at + SUB, :] = pltpu.roll(turned(next_m), width - 1, 1)
            tiles[0].append(jnp.where(lane < steps, turned(near) - jnp.log(incoming), 0.0))
            tiles[1].append(jnp.where(lane < steps, incoming * turned(far), 0.0))
    target = lax.broadcasted_iota(jnp.int32, (2 * width, width), 1)
    columns[...] = jnp.zeros_like(columns)
    for kind, shift in enumerate((width - 1, 0)):
        place = ((2 * rows + shift) % width == target) & (rows < steps)
        place = jnp.where(place, 1.0, 0.0).astype(jnp.bfloat16)
        columns[...] += jnp.dot(halves(jnp.concatenate(tiles[kind], axis=0)), place, preferred_element_type=jnp.float32)
    state_ref[...] = jnp.zeros_like(state_ref)
    front[...] = jnp.ones_like(front)
    field[:, width_a:, :] = jnp.zeros((4, SUB, width), jnp.float32)
    lane = lax.broadcasted_iota(jnp.int32, (BAND, width), 1)
    last = lane == width - 1
    zeroth = lane == 0

    def slice_of(b, behind):
        if not behind:
            for fetch in fetches(b):
                fetch.wait()
        joined = []
        for start in range(0, width_a, BAND):
            at = slice(start, start + BAND)
            masked = brim_ref[0, at, :] if behind else density[b, at, :] * mask[at, :]
            field[0, at, :] = masked
            field[2, at, :] = jnp.where(last, edges[at, :], pltpu.roll(masked, width - 1, 1))
            joined.append(halves(jnp.where(last, columns[at, :], masked)))
            edges[at, :] = pltpu.roll(edges[at, :], width - 1, 1)
        within = jnp.dot(jnp.concatenate(joined, axis=0), tri[...], preferred_element_type=jnp.float32)
        for start in range(0, width_a, BAND):
            at = slice(start, start + BAND)
            lit = (brim_ref[1, at, :] if behind else albedo[b, at, :]) * jnp.exp(-within[at])
            spot = columns[at, :]
            field[1, at, :] = lit
            field[3, at, :] = pltpu.roll(jnp.where(zeroth, spot, lit), width - 1, 1)
            columns[at, :] = pltpu.roll(spot, width - 2, 1)
        started = b > 0
        for start in range(0, width_a, BAND):
            at = slice(start, start + BAND)
            below = slice(start + 1, start + BAND + 1)
            corner = [weights[i, at, :] for i in range(4)]

            def mixed(kind):
                return (corner[0] * field[kind, at, :] + corner[1] * field[kind, below, :]) + (
                    corner[2] * field[kind + 2, at, :] + corner[3] * field[kind + 2, below, :]
                )

            mix_m = mixed(0)
            mix_s = mixed(1)
            old_m = state_ref[2, at, :]
            old_s = state_ref[3, at, :]
            depth_w = depth_ref[at, :]
            extinct = jnp.where(started, old_m + depth_w * (mix_m - old_m), 0.0)
            shaded = old_s + depth_w * (mix_s - old_s)
            total = state_ref[1, at, :] + extinct
            left = jnp.exp(-total)
            state_ref[0, at, :] = state_ref[0, at, :] + (front[at, :] - left) * shaded
            state_ref[1, at, :] = total
            front[at, :] = left
            state_ref[2, at, :] = mix_m
            state_ref[3, at, :] = mix_s

    def two_slices(pair, _):
        slice_of(2 * pair, False)
        slice_of(2 * pair + 1, False)
        return 0

    lax.fori_loop(0, depth // 2, two_slices, 0)
    slice_of(depth, True)
    rows = out_ref.shape[2]
    for chunk in range(out_ref.shape[0]):
        out_ref[chunk] = state_ref[:2, chunk * rows : (chunk + 1) * rows, :]


def march(density, albedo, light_cols, brim, occupancy, fractions, small, others, rays, screens):
    depth, width_a, width = density.shape
    vmem = pl.BlockSpec(memory_space=pltpu.VMEM)
    hbm = pl.BlockSpec(memory_space=pl.ANY)
    others = [pltpu.with_memory_space_constraint(x, pltpu.HBM) for x in others]
    plane = pltpu.VMEM((width_a, width), jnp.float32)
    return pl.pallas_call(
        functools.partial(march_kernel, len(others) + 1),
        in_specs=[hbm, pl.BlockSpec(memory_space=pltpu.SMEM), hbm, hbm, hbm, vmem, vmem] + [hbm] * len(others) + [vmem],
        out_specs=vmem,
        scratch_shapes=[
            pltpu.VMEM((4, width_a, width), jnp.float32),
            plane,
            pltpu.VMEM((occupancy.shape[2], width), jnp.float32),
            plane,
            plane,
            plane,
            pltpu.VMEM((4, width_a, width), jnp.float32),
            plane,
            pltpu.VMEM((2 * width, width), jnp.bfloat16),
            pltpu.VMEM((4, width_a + SUB, width), jnp.float32),
            pltpu.VMEM(density.shape, jnp.float32),
            pltpu.VMEM(density.shape, jnp.float32),
            pltpu.VMEM(occupancy.shape, occupancy.dtype),
            pltpu.VMEM(light_cols.shape, jnp.float32),
            pltpu.VMEM((len(others), *small.shape), jnp.float32),
            pltpu.SemaphoreType.DMA((3, max(depth, 2 + len(others)))),
        ],
        out_shape=jax.ShapeDtypeStruct((screens, 2, width_a // screens, width), jnp.float32),
        compiler_params=pltpu.CompilerParams(vmem_limit_bytes=MARCH_VMEM),
        cost_estimate=pl.CostEstimate(flops=10**8, bytes_accessed=2 * depth * width_a * width * 4, transcendentals=0),
        name="march",
    )(occupancy, fractions, density, albedo, light_cols, brim, small, *others, rays)


def shifted(value, axis, by):
    peers = lax.axis_size(axis)
    return lax.ppermute(value, axis, [(i, i + by) for i in range(peers) if 0 <= i + by < peers])


def swapped(value, axis, by):
    peers = lax.axis_size(axis)
    return lax.ppermute(value, axis, [(i, i ^ by) for i in range(peers)])


def step(density, albedo, light_in, occupancy, phase, fractions):
    depth, width_a, width = density.shape
    lights, screens = lax.axis_size("light"), lax.axis_size("screen")
    light, screen = lax.axis_index("light"), lax.axis_index("screen")
    per = screens // lights
    rows = width_a // screens
    rounds = rounds_of(lights, screens)
    pairs = [round_pairs(rnd, lights, screens) for rnd in rounds]

    def spot_of(j):
        here = lax.axis_index("light"), lax.axis_index("screen")
        return target_screen(*here, (lax.rem(j, lights), lax.div(j, lights)), lights, screens)

    def place_of(j):
        return source_of(lax.axis_index("light"), lax.axis_index("screen"), rounds[j], lights, screens)

    def send(j, chunk):
        return lax.ppermute(chunk, ("light", "screen"), pairs[j])

    count = len(rounds)
    flags = pltpu.with_memory_space_constraint(occupancy.transpose(0, 2, 1), pltpu.HBM)
    density = pltpu.with_memory_space_constraint(density, pltpu.HBM)
    albedo = pltpu.with_memory_space_constraint(albedo, pltpu.HBM)
    early = lit_chunks(density, albedo, flags, spot_of, 0, 2, screens)
    late = lit_chunks(density, albedo, flags, spot_of, 2, count - 2, screens, early[-1])
    arrived = [send(j, chunk) for j, chunk in enumerate(early[:2] + late[:-1])]
    brim = shifted(early[2], "screen", -1)
    small = with_rim(late[-1], brim, depth)
    others = [swapped(small, "light", by) for by in range(1, lights)]
    light_cols = jnp.pad(light_in, ((0, 1), (0, 0)), constant_values=1.0)
    light_cols = lax.dynamic_slice_in_dim(light_cols, screen * depth, depth + 1, 0).T
    rays = lax.dynamic_slice_in_dim(phase, light * width, width, 1)
    parts = march(density, albedo, light_cols, brim, flags, fractions, small, others, rays, screens)
    got = lax.all_to_all(parts, "screen", split_axis=0, concat_axis=0, tiled=True)
    incoming = lax.dynamic_slice(light_in, (light * per * depth, screen * rows), (per * depth, rows))
    incoming = jnp.pad(incoming.reshape(per, depth, rows // SUB, SUB), ((0, 0), (0, 1), (0, 0), (0, 0)))
    incoming = incoming.transpose(0, 3, 2, 1).reshape(per, SUB, rows // SUB * (depth + 1))
    incoming = jnp.pad(incoming, ((0, 0), (0, 0), (0, width - incoming.shape[2])))
    return gather_block(arrived, got, incoming, place_of, depth, lights, per)


def local(*args):
    return tuple(step(*args))


def solution(mesh):
    return jax.shard_map(
        local,
        mesh=mesh,
        in_specs=(
            P("screen", None, "light"),
            P("screen", None, "light"),
            P(),
            P("screen", None, "light"),
            P(),
            P(),
        ),
        out_specs=(P("screen", "light"), P("screen", "light"), P("light", "screen", None)),
        check_vma=False,
    )
```

```python
import functools

import jax
import jax.numpy as jnp
from jax import lax
from jax.experimental import pallas as pl
from jax.experimental.pallas import tpu as pltpu
from jax.sharding import PartitionSpec as P


BRICK = 16
SUB = 8


def bit_reversed(value, size):
    out = 0
    bit = 1
    while bit < size:
        out = out * 2 + ((value // bit) & 1 if isinstance(value, int) else lax.div(value, bit) & 1)
        bit *= 2
    return out


def over(value, by):
    return value // by if isinstance(value, int) else lax.div(value, by)


def rounds_of(lights, screens):
    per = screens // lights
    return [(step, core) for core in range(per) for step in range(lights)]


def target_screen(light, screen, rnd, lights, screens):
    per = screens // lights
    step, core = rnd
    return (bit_reversed(over(screen, per), lights) ^ light ^ step) * per + ((screen & (per - 1)) ^ core)


def source_of(light, screen, rnd, lights, screens):
    per = screens // lights
    step, core = rnd
    return bit_reversed(light, lights) ^ over(screen, per) ^ step, (screen & (per - 1)) ^ core


def round_pairs(rnd, lights, screens):
    per = screens // lights
    pairs = []
    for light in range(lights):
        for screen in range(screens):
            there = (screen // per) * screens + target_screen(light, screen, rnd, lights, screens)
            pairs.append((light * screens + screen, there))
    return pairs


def brick_rows(occ_ref, out, width):
    bricks = occ_ref.shape[1]
    here = lax.broadcasted_iota(jnp.int32, (bricks, width), 1) // BRICK
    spread = (here == lax.broadcasted_iota(jnp.int32, (bricks, width), 0)).astype(jnp.float32)
    flags = occ_ref[0].astype(jnp.float32)
    out[...] = lax.dot_general(flags, spread, (((0,), (0,)), ((), ())), preferred_element_type=jnp.float32)


def halves(values):
    high = values.astype(jnp.bfloat16)
    low = (values - high.astype(jnp.float32)).astype(jnp.bfloat16)
    return jnp.concatenate([high, low], axis=-1)


def prefix_matrix(width, with_total):
    rows = lax.broadcasted_iota(jnp.int32, (2 * width, (1 + with_total) * width), 0) % width
    cols = lax.broadcasted_iota(jnp.int32, (2 * width, (1 + with_total) * width), 1)
    return (rows < cols).astype(jnp.float32).astype(jnp.bfloat16)


def chunk_kernel(count, spot_of, first, *refs):
    occ_any, density_ref, albedo_ref = refs[:3]
    before = refs[3 : 3 + bool(first)]
    rest = refs[3 + bool(first) :]
    outs = rest[:count]
    brims = rest[count : -7]
    small_ref, occ_ref, brick, tri, density, albedo, sem = rest[-7:]
    _, depth, rows, width = density.shape

    def fetches(k):
        columns = pl.ds(spot_of(first + k) * rows, rows)
        return (
            pltpu.make_async_copy(density_ref.at[:, columns, :], density.at[k], sem.at[0, k]),
            pltpu.make_async_copy(albedo_ref.at[:, columns, :], albedo.at[k], sem.at[1, k]),
        )

    flags = pltpu.make_async_copy(occ_any, occ_ref, sem.at[2, 0])
    flags.start()
    for k in range(count):
        for fetch in fetches(k):
            fetch.start()
    for brim in brims:
        pltpu.make_async_copy(density_ref.at[0], brim.at[0], sem.at[2, 1]).start()
        pltpu.make_async_copy(albedo_ref.at[0], brim.at[1], sem.at[2, 2]).start()
    tri[...] = prefix_matrix(width, 1)
    flags.wait()
    brick_rows(occ_ref, brick, width)
    bands = rows // BRICK
    lane = lax.broadcasted_iota(jnp.int32, (SUB, width), 1)
    for k in range(count):
        spot = spot_of(first + k)
        mask = jnp.concatenate(
            [jnp.broadcast_to(brick[pl.ds(spot * bands + band, 1), :], (BRICK, width)) for band in range(bands)], axis=0
        )
        for fetch in fetches(k):
            fetch.wait()
        packed = [jnp.zeros((SUB, width), jnp.float32)] * 3
        for b in range(depth):
            masked = density[k, b] * mask
            sums = jnp.dot(halves(masked), tri[...], preferred_element_type=jnp.float32)
            light = albedo[k, b]
            outs[k][b * rows : (b + 1) * rows, :] = light * jnp.exp(-sums[:, :width])
            for group in range(rows // SUB):
                at = slice(group * SUB, (group + 1) * SUB)
                here = lane == group * (depth + 1) + b
                packed[0] = jnp.where(here, sums[at, width:], packed[0])
                packed[1] = jnp.where(here, masked[at, 0:1], packed[1])
                packed[2] = jnp.where(here, light[at, 0:1], packed[2])
        outs[k][depth * rows :, :] = packed[0]
        tile = pl.multiple_of(spot * SUB, SUB) if first else k * SUB
        for kind in range(3):
            small_ref[kind, pl.ds(tile, SUB), :] = packed[kind]
    for brim in brims:
        pltpu.make_async_copy(density_ref.at[0], brim.at[0], sem.at[2, 1]).wait()
        pltpu.make_async_copy(albedo_ref.at[0], brim.at[1], sem.at[2, 2]).wait()
        for row in range(brick.shape[0]):
            at = slice(row * BRICK, (row + 1) * BRICK)
            brim[0, at, :] = brim[0, at, :] * brick[row : row + 1, :]
    for held in before:
        for k in range(first):
            tile = pl.multiple_of(spot_of(k) * SUB, SUB)
            small_ref[:, pl.ds(tile, SUB), :] = held[:, k * SUB : (k + 1) * SUB, :]


def lit_chunks(density, albedo, occupancy, spot_of, first, count, screens, *before):
    depth, width_a, width = density.shape
    rows = width_a // screens
    size = depth * rows + SUB
    vmem = pl.BlockSpec(memory_space=pltpu.VMEM)
    tiles = screens if before else count
    brim = [] if before else [jax.ShapeDtypeStruct((2, width_a, width), jnp.float32)]
    return pl.pallas_call(
        functools.partial(chunk_kernel, count, spot_of, first),
        in_specs=[pl.BlockSpec(memory_space=pl.ANY)] * 3 + [vmem] * len(before),
        out_specs=[vmem] * (count + 1 + len(brim)),
        out_shape=[jax.ShapeDtypeStruct((size, width), jnp.float32)] * count
        + brim
        + [jax.ShapeDtypeStruct((3, SUB * tiles, width), jnp.float32)],
        scratch_shapes=[
            pltpu.VMEM(occupancy.shape, occupancy.dtype),
            pltpu.VMEM((occupancy.shape[2], width), jnp.float32),
            pltpu.VMEM((2 * width, 2 * width), jnp.bfloat16),
            pltpu.VMEM((count, depth, rows, width), jnp.float32),
            pltpu.VMEM((count, depth, rows, width), jnp.float32),
            pltpu.SemaphoreType.DMA((3, max(count, 3))),
        ],
        compiler_params=pltpu.CompilerParams(vmem_limit_bytes=CHUNK_VMEM),
        cost_estimate=pl.CostEstimate(flops=10**7 * count, bytes_accessed=3 * size * width * 4 * count, transcendentals=0),
        name="lit_chunks",
    )(occupancy, density, albedo, *before)


CHUNK_VMEM = 12 << 20
MARCH_VMEM = 16 << 20


def rim_kernel(depth, small_ref, brim_ref, out_ref):
    _, width_a, width = brim_ref.shape
    tiles = small_ref.shape[1] // SUB
    groups = width_a // tiles // SUB
    masked = brim_ref[0]
    light = brim_ref[1]
    total = jnp.dot(halves(masked), jnp.ones((2 * width, width), jnp.bfloat16), preferred_element_type=jnp.float32)
    lane = lax.broadcasted_iota(jnp.int32, (SUB, width), 1)
    for tile in range(tiles):
        rows = slice(tile * SUB, (tile + 1) * SUB)
        packed = [small_ref[kind, rows, :] for kind in range(3)]
        for group in range(groups):
            at = slice((tile * groups + group) * SUB, (tile * groups + group + 1) * SUB)
            here = lane == group * (depth + 1) + depth
            packed[0] = jnp.where(here, total[at], packed[0])
            packed[1] = jnp.where(here, masked[at, 0:1], packed[1])
            packed[2] = jnp.where(here, light[at, 0:1], packed[2])
        for kind in range(3):
            out_ref[kind, rows, :] = packed[kind]


def with_rim(small, brim, depth):
    vmem = pl.BlockSpec(memory_space=pltpu.VMEM)
    return pl.pallas_call(
        functools.partial(rim_kernel, depth),
        in_specs=[vmem] * 2,
        out_specs=vmem,
        out_shape=jax.ShapeDtypeStruct(small.shape, jnp.float32),
        compiler_params=pltpu.CompilerParams(vmem_limit_bytes=4 << 20),
        cost_estimate=pl.CostEstimate(flops=10**6, bytes_accessed=10**6, transcendentals=0),
        name="rim",
    )(small, brim)


def gather_kernel(depth, lights, place_of, light_ref, parts_ref, *refs):
    count = len(refs) - 6
    chunks = refs[:count]
    image_ref, through_ref, out_ref, held, totals, sem = refs[count:]
    size, width = chunks[0].shape
    rows = (size - SUB) // depth
    for j in range(count):
        light, place = place_of(j)
        totals[place, light] = chunks[j][size - SUB :, :]
    copies = []
    for j in range(count):
        light, place = place_of(j)
        before = jnp.zeros((SUB, width), jnp.float32)
        for other in range(lights - 1):
            before = before + jnp.where(other < light, totals[place, other], 0.0)
        factor = light_ref[place] * jnp.exp(-before)
        for b in range(depth):
            for group in range(rows // SUB):
                at = b * rows + group * SUB
                lane = group * (depth + 1) + b
                held[j, b, group * SUB : (group + 1) * SUB, :] = chunks[j][at : at + SUB, :] * factor[:, lane : lane + 1]
        copy = pltpu.make_async_copy(
            held.at[j],
            out_ref.at[pl.ds(place * depth, depth), :, pl.ds(pl.multiple_of(light * width, width), width)],
            sem.at[j],
        )
        copy.start()
        copies.append(copy)
    image = jnp.zeros(image_ref.shape, jnp.float32)
    ahead = jnp.zeros(image_ref.shape, jnp.float32)
    for slab in range(parts_ref.shape[0]):
        image = image + jnp.exp(-ahead) * parts_ref[slab, 0]
        ahead = ahead + parts_ref[slab, 1]
    image_ref[...] = image
    through_ref[...] = jnp.exp(-ahead)
    for copy in copies:
        copy.wait()


def gather_block(chunks, parts, incoming, place_of, depth, lights, per):
    size, width = chunks[0].shape
    rows = (size - SUB) // depth
    return pl.pallas_call(
        functools.partial(gather_kernel, depth, lights, place_of),
        in_specs=[pl.BlockSpec(memory_space=pltpu.VMEM)] * (2 + len(chunks)),
        out_specs=[pl.BlockSpec(memory_space=pltpu.VMEM)] * 2 + [pl.BlockSpec(memory_space=pl.ANY)],
        out_shape=[jax.ShapeDtypeStruct((rows, width), jnp.float32)] * 2
        + [jax.ShapeDtypeStruct((per * depth, rows, lights * width), jnp.float32)],
        scratch_shapes=[
            pltpu.VMEM((len(chunks), depth, rows, width), jnp.float32),
            pltpu.VMEM((per, lights, SUB, width), jnp.float32),
            pltpu.SemaphoreType.DMA((len(chunks),)),
        ],
        compiler_params=pltpu.CompilerParams(vmem_limit_bytes=24 << 20),
        name="gather_block",
    )(incoming, parts, *chunks)


BAND = 32


def march_kernel(lights, occ_any, frac_ref, density_ref, albedo_ref, light_any, brim_ref, small_ref, *refs):
    arriving = refs[: lights - 1]
    phase_ref, out_ref = refs[lights - 1 : lights + 1]
    state_ref, depth_ref, brick, mask, columns, edges, weights, front, tri, field = refs[lights + 1 : lights + 11]
    density, albedo, occ_ref, light_ref, others, sem = refs[lights + 11 :]
    depth, width_a, width = density.shape
    steps = light_ref.shape[1]

    def fetches(b):
        return (
            pltpu.make_async_copy(density_ref.at[b], density.at[b], sem.at[0, b]),
            pltpu.make_async_copy(albedo_ref.at[b], albedo.at[b], sem.at[1, b]),
        )

    early = [pltpu.make_async_copy(occ_any, occ_ref, sem.at[2, 0]), pltpu.make_async_copy(light_any, light_ref, sem.at[2, 1])]
    early += [pltpu.make_async_copy(ref, others.at[i], sem.at[2, 2 + i]) for i, ref in enumerate(arriving)]
    for copy in early:
        copy.start()
    for b in range(depth):
        for fetch in fetches(b):
            fetch.start()
    for start in range(0, width_a, BAND):
        at = slice(start, start + BAND)
        levels = phase_ref[at, :]
        picked = [jnp.zeros((BAND, width), jnp.float32)] * 3
        for level in range(frac_ref.shape[1]):
            here = levels == level
            picked = [jnp.where(here, frac_ref[axis, level], value) for axis, value in enumerate(picked)]
        depth_ref[at, :] = picked[0]
        far_w = picked[1] * picked[2]
        weights[0, at, :] = 1.0 - picked[1] - picked[2] + far_w
        weights[1, at, :] = picked[1] - far_w
        weights[2, at, :] = picked[2] - far_w
        weights[3, at, :] = far_w
    rows = lax.broadcasted_iota(jnp.int32, (2 * width, width), 0) % width
    above = rows < lax.broadcasted_iota(jnp.int32, (2 * width, width), 1)
    tri[...] = jnp.where(above | (rows == width - 1), 1.0, 0.0).astype(jnp.bfloat16)
    for copy in early:
        copy.wait()
    brick_rows(occ_ref, brick, width)
    for row in range(width_a // BRICK):
        mask[row * BRICK : (row + 1) * BRICK, :] = jnp.broadcast_to(brick[row : row + 1, :], (BRICK, width))
    light = lax.axis_index("light")
    near = jnp.zeros(small_ref.shape[1:], jnp.float32)
    next_m = jnp.zeros(small_ref.shape[1:], jnp.float32)
    next_a = jnp.zeros(small_ref.shape[1:], jnp.float32)
    for by in range(1, lights):
        other = light ^ by
        near = near + jnp.where(other < light, others[by - 1, 0], 0.0)
        next_m = next_m + jnp.where(other == light + 1, others[by - 1, 1], 0.0)
        next_a = next_a + jnp.where(other == light + 1, others[by - 1, 2], 0.0)
    far = jnp.exp(-(near + small_ref[0])) * next_a
    chunks = near.shape[0] // SUB
    groups = width_a // chunks // SUB
    lane = lax.broadcasted_iota(jnp.int32, (SUB, width), 1)
    tiles = [[], []]
    for chunk in range(chunks):
        for group in range(groups):
            at = (chunk * groups + group) * SUB
            back = (width - group * steps) % width

            def turned(x):
                tile = x[chunk * SUB : (chunk + 1) * SUB]
                return pltpu.roll(tile, back, 1) if back else tile

            incoming = jnp.concatenate([light_ref[at : at + SUB, :], jnp.ones((SUB, width - steps), jnp.float32)], axis=1)
            edges[at : at + SUB, :] = pltpu.roll(turned(next_m), width - 1, 1)
            tiles[0].append(jnp.where(lane < steps, turned(near) - jnp.log(incoming), 0.0))
            tiles[1].append(jnp.where(lane < steps, incoming * turned(far), 0.0))
    target = lax.broadcasted_iota(jnp.int32, (2 * width, width), 1)
    columns[...] = jnp.zeros_like(columns)
    for kind, shift in enumerate((width - 1, 0)):
        place = ((2 * rows + shift) % width == target) & (rows < steps)
        place = jnp.where(place, 1.0, 0.0).astype(jnp.bfloat16)
        columns[...] += jnp.dot(halves(jnp.concatenate(tiles[kind], axis=0)), place, preferred_element_type=jnp.float32)
    state_ref[...] = jnp.zeros_like(state_ref)
    front[...] = jnp.ones_like(front)
    field[:, width_a:, :] = jnp.zeros((4, SUB, width), jnp.float32)
    lane = lax.broadcasted_iota(jnp.int32, (BAND, width), 1)
    last = lane == width - 1
    zeroth = lane == 0

    def slice_of(b, behind):
        if not behind:
            for fetch in fetches(b):
                fetch.wait()
        joined = []
        for start in range(0, width_a, BAND):
            at = slice(start, start + BAND)
            masked = brim_ref[0, at, :] if behind else density[b, at, :] * mask[at, :]
            field[0, at, :] = masked
            field[2, at, :] = jnp.where(last, edges[at, :], pltpu.roll(masked, width - 1, 1))
            joined.append(halves(jnp.where(last, columns[at, :], masked)))
            edges[at, :] = pltpu.roll(edges[at, :], width - 1, 1)
        within = jnp.dot(jnp.concatenate(joined, axis=0), tri[...], preferred_element_type=jnp.float32)
        for start in range(0, width_a, BAND):
            at = slice(start, start + BAND)
            lit = (brim_ref[1, at, :] if behind else albedo[b, at, :]) * jnp.exp(-within[at])
            spot = columns[at, :]
            field[1, at, :] = lit
            field[3, at, :] = pltpu.roll(jnp.where(zeroth, spot, lit), width - 1, 1)
            columns[at, :] = pltpu.roll(spot, width - 2, 1)
        started = b > 0
        for start in range(0, width_a, BAND):
            at = slice(start, start + BAND)
            below = slice(start + 1, start + BAND + 1)
            corner = [weights[i, at, :] for i in range(4)]

            def mixed(kind):
                return (corner[0] * field[kind, at, :] + corner[1] * field[kind, below, :]) + (
                    corner[2] * field[kind + 2, at, :] + corner[3] * field[kind + 2, below, :]
                )

            mix_m = mixed(0)
            mix_s = mixed(1)
            old_m = state_ref[2, at, :]
            old_s = state_ref[3, at, :]
            depth_w = depth_ref[at, :]
            extinct = jnp.where(started, old_m + depth_w * (mix_m - old_m), 0.0)
            shaded = old_s + depth_w * (mix_s - old_s)
            total = state_ref[1, at, :] + extinct
            left = jnp.exp(-total)
            state_ref[0, at, :] = state_ref[0, at, :] + (front[at, :] - left) * shaded
            state_ref[1, at, :] = total
            front[at, :] = left
            state_ref[2, at, :] = mix_m
            state_ref[3, at, :] = mix_s

    def two_slices(pair, _):
        slice_of(2 * pair, False)
        slice_of(2 * pair + 1, False)
        return 0

    lax.fori_loop(0, depth // 2, two_slices, 0)
    slice_of(depth, True)
    rows = out_ref.shape[2]
    for chunk in range(out_ref.shape[0]):
        out_ref[chunk] = state_ref[:2, chunk * rows : (chunk + 1) * rows, :]


def march(density, albedo, light_cols, brim, occupancy, fractions, small, others, rays, screens):
    depth, width_a, width = density.shape
    vmem = pl.BlockSpec(memory_space=pltpu.VMEM)
    hbm = pl.BlockSpec(memory_space=pl.ANY)
    others = [pltpu.with_memory_space_constraint(x, pltpu.HBM) for x in others]
    plane = pltpu.VMEM((width_a, width), jnp.float32)
    return pl.pallas_call(
        functools.partial(march_kernel, len(others) + 1),
        in_specs=[hbm, pl.BlockSpec(memory_space=pltpu.SMEM), hbm, hbm, hbm, vmem, vmem] + [hbm] * len(others) + [vmem],
        out_specs=vmem,
        scratch_shapes=[
            pltpu.VMEM((4, width_a, width), jnp.float32),
            plane,
            pltpu.VMEM((occupancy.shape[2], width), jnp.float32),
            plane,
            plane,
            plane,
            pltpu.VMEM((4, width_a, width), jnp.float32),
            plane,
            pltpu.VMEM((2 * width, width), jnp.bfloat16),
            pltpu.VMEM((4, width_a + SUB, width), jnp.float32),
            pltpu.VMEM(density.shape, jnp.float32),
            pltpu.VMEM(density.shape, jnp.float32),
            pltpu.VMEM(occupancy.shape, occupancy.dtype),
            pltpu.VMEM(light_cols.shape, jnp.float32),
            pltpu.VMEM((len(others), *small.shape), jnp.float32),
            pltpu.SemaphoreType.DMA((3, max(depth, 2 + len(others)))),
        ],
        out_shape=jax.ShapeDtypeStruct((screens, 2, width_a // screens, width), jnp.float32),
        compiler_params=pltpu.CompilerParams(vmem_limit_bytes=MARCH_VMEM),
        cost_estimate=pl.CostEstimate(flops=10**8, bytes_accessed=2 * depth * width_a * width * 4, transcendentals=0),
        name="march",
    )(occupancy, fractions, density, albedo, light_cols, brim, small, *others, rays)


def shifted(value, axis, by):
    peers = lax.axis_size(axis)
    return lax.ppermute(value, axis, [(i, i + by) for i in range(peers) if 0 <= i + by < peers])


def swapped(value, axis, by):
    peers = lax.axis_size(axis)
    return lax.ppermute(value, axis, [(i, i ^ by) for i in range(peers)])


def step(density, albedo, light_in, occupancy, phase, fractions):
    depth, width_a, width = density.shape
    lights, screens = lax.axis_size("light"), lax.axis_size("screen")
    light, screen = lax.axis_index("light"), lax.axis_index("screen")
    per = screens // lights
    rows = width_a // screens
    rounds = rounds_of(lights, screens)
    pairs = [round_pairs(rnd, lights, screens) for rnd in rounds]

    def spot_of(j):
        here = lax.axis_index("light"), lax.axis_index("screen")
        return target_screen(*here, (lax.rem(j, lights), lax.div(j, lights)), lights, screens)

    def place_of(j):
        return source_of(lax.axis_index("light"), lax.axis_index("screen"), rounds[j], lights, screens)

    def send(j, chunk):
        return lax.ppermute(chunk, ("light", "screen"), pairs[j])

    count = len(rounds)
    flags = pltpu.with_memory_space_constraint(occupancy.transpose(0, 2, 1), pltpu.HBM)
    density = pltpu.with_memory_space_constraint(density, pltpu.HBM)
    albedo = pltpu.with_memory_space_constraint(albedo, pltpu.HBM)
    early = lit_chunks(density, albedo, flags, spot_of, 0, 3, screens)
    late = lit_chunks(density, albedo, flags, spot_of, 3, count - 3, screens, early[-1])
    arrived = [send(j, chunk) for j, chunk in enumerate(early[:3] + late[:-1])]
    brim = shifted(early[3], "screen", -1)
    small = with_rim(late[-1], brim, depth)
    others = [swapped(small, "light", by) for by in range(1, lights)]
    light_cols = jnp.pad(light_in, ((0, 1), (0, 0)), constant_values=1.0)
    light_cols = lax.dynamic_slice_in_dim(light_cols, screen * depth, depth + 1, 0).T
    rays = lax.dynamic_slice_in_dim(phase, light * width, width, 1)
    parts = march(density, albedo, light_cols, brim, flags, fractions, small, others, rays, screens)
    got = lax.all_to_all(parts, "screen", split_axis=0, concat_axis=0, tiled=True)
    incoming = lax.dynamic_slice(light_in, (light * per * depth, screen * rows), (per * depth, rows))
    incoming = jnp.pad(incoming.reshape(per, depth, rows // SUB, SUB), ((0, 0), (0, 1), (0, 0), (0, 0)))
    incoming = incoming.transpose(0, 3, 2, 1).reshape(per, SUB, rows // SUB * (depth + 1))
    incoming = jnp.pad(incoming, ((0, 0), (0, 0), (0, width - incoming.shape[2])))
    return gather_block(arrived, got, incoming, place_of, depth, lights, per)


def local(*args):
    return tuple(step(*args))


def solution(mesh):
    return jax.shard_map(
        local,
        mesh=mesh,
        in_specs=(
            P("screen", None, "light"),
            P("screen", None, "light"),
            P(),
            P("screen", None, "light"),
            P(),
            P(),
        ),
        out_specs=(P("screen", "light"), P("screen", "light"), P("light", "screen", None)),
        check_vma=False,
    )
```
